32 devices in a mesh: rows: 8 (over z, y), cols: 4 (over x, core).
Axes of the slice: x: 2, y: 2, z: 4, core: 2. Of those that a mesh axis runs over, the one named last changes fastest.
Arguments:
- orthophoto: float32 [3, 1024, 2048], P(None, 'rows', 'cols'), may hold values from 0 to 1
Outputs:
- detail_zero: float32 [3, 1024, 2048], P(None, 'rows', 'cols')
- detail_one: float32 [3, 512, 1024], P(None, 'rows', 'cols')
- detail_two: float32 [3, 256, 512], P(None, 'rows', 'cols')
- detail_three: float32 [3, 128, 256], P(None, 'rows', 'cols')
- detail_four: float32 [3, 64, 128], P(None, 'rows', 'cols')
- coarsest: float32 [3, 32, 64], P(None, 'rows', 'cols')
The draws below stay inside these ranges and needn't reach their ends.
All inputs are finite; a program needn't handle non-finite values.
Results may differ from the reference program's by a relative error of at most 0.00015.
Values sent between devices are 32-bit elements; how exact they have to be, the bound alone decides.
A program may use at most 64 MiB of HBM per device.

```python
import jax
import jax.numpy as jnp
from jax import lax

CHANNELS = 3
LEVELS = 5
NROWS = 1024
NCOLS = 2048


def steps_of(rng, dims, pieces, least, top_value):
    def one(position, shards_of):
        heights = jax.random.uniform(jax.random.fold_in(jax.random.fold_in(rng, 6), position), (shards_of,), jnp.float32, least / len(pieces), top_value / len(pieces))
        return jnp.repeat(jnp.exp(heights), dims[position] // shards_of).reshape((-1,) + (1,) * (len(dims) - position - 1))

    gain = one(*pieces[0])
    for cut in pieces[1:]:
        gain = gain * one(*cut)
    return gain


def setup_inputs(seed: int = 0) -> dict:
    key_list = jax.random.split(jax.random.key(seed), 2)
    return {
        "orthophoto": jnp.clip(1.0 * jax.random.uniform(key_list[0], (CHANNELS, NROWS, NCOLS), jnp.float32) ** steps_of(key_list[0], (CHANNELS, NROWS, NCOLS), ((1, 8), (2, 4)), -0.2, 0.2), 0.0, 1.0),
    }


TAPS = (0.0625, 0.25, 0.375, 0.25, 0.0625)


def decimate(padded, axis_dim, out_count):
    summed = TAPS[0] * lax.slice_in_dim(padded, 0, 2 * out_count - 1, 2, axis_dim)
    for tap_index in range(1, 5):
        summed = summed + TAPS[tap_index] * lax.slice_in_dim(padded, tap_index, tap_index + 2 * out_count - 1, 2, axis_dim)
    return summed


def shrink(current):
    padded = jnp.pad(current, ((0, 0), (2, 2), (2, 2)), mode="reflect")
    vertical = decimate(padded, 1, current.shape[1] // 2)
    return decimate(vertical, 2, current.shape[2] // 2)


def alternate(even_part, odd_part, axis_dim):
    stacked = jnp.stack([even_part, odd_part], axis=axis_dim + 1)
    new_shape = list(even_part.shape)
    new_shape[axis_dim] = 2 * new_shape[axis_dim]
    return stacked.reshape(new_shape)


def upsample(bordered, axis_dim):
    inner_count = bordered.shape[axis_dim] - 2
    before = lax.slice_in_dim(bordered, 0, inner_count, 1, axis_dim)
    center = lax.slice_in_dim(bordered, 1, inner_count + 1, 1, axis_dim)
    after = lax.slice_in_dim(bordered, 2, inner_count + 2, 1, axis_dim)
    return alternate((before + 6.0 * center + after) * 0.125, (center + after) * 0.5, axis_dim)


def expand(bordered):
    return upsample(upsample(bordered, 1), 2)


def pad_coarse(coarse, axis_dim):
    inner_count = coarse.shape[axis_dim]
    head_cell = lax.slice_in_dim(coarse, 1, 2, 1, axis_dim)
    tail_cell = lax.slice_in_dim(coarse, inner_count - 1, inner_count, 1, axis_dim)
    return jnp.concatenate([head_cell, coarse, tail_cell], axis=axis_dim)


def encode_plane(plane):
    current = plane[None]
    details = []
    for layer_index in range(LEVELS):
        coarse = shrink(current)
        bordered = pad_coarse(pad_coarse(coarse, 1), 2)
        details.append(current - expand(bordered))
        current = coarse
    return (details[0][0], details[1][0], details[2][0], details[3][0], details[4][0], current[0])


def reference(orthophoto):
    results = lax.map(encode_plane, orthophoto)
    return (results[0], results[1], results[2], results[3], results[4], results[5])
```

```python
import functools

import jax
import jax.numpy as jnp
from jax import lax
from jax.experimental import pallas as pl
from jax.experimental.pallas import tpu as pltpu
from jax.sharding import PartitionSpec as P

LEVELS = 5
LANES = 128
EDGE = 8
ABOVE, BELOW = 24, 16
BF16 = jnp.bfloat16
F32 = jnp.float32
MESH = pl.DeviceIdType.MESH
DIRECTIONS = ((-1, 0), (1, 0), (0, -1), (0, 1), (-1, -1), (-1, 1), (1, -1), (1, 1))


def pitch(width):
    return width + LANES if width >= LANES else LANES


def local_of(lane, width, total):
    return jnp.where(lane < width + (total - width) // 2, lane, lane - total)


def reduce_tap(distance):
    far = jnp.abs(distance)
    return jnp.where(far == 0, 0.375, jnp.where(far == 1, 0.25, jnp.where(far == 2, 0.0625, 0.0)))


def expand_tap(distance):
    far = jnp.abs(distance)
    return jnp.where(far == 0, 0.75, jnp.where(far == 1, 0.5, jnp.where(far == 2, 0.125, 0.0)))


def fill_weights(ref, col, in_width, in_cols, out_width, out_halo, expanding):
    in_total, out_total = ref.shape
    chunk = 32

    def one(step, carry):
        base = step * chunk
        lane_in = base + lax.broadcasted_iota(jnp.int32, (chunk, out_total), 0)
        lane_out = lax.broadcasted_iota(jnp.int32, (chunk, out_total), 1)
        g = local_of(lane_in, in_width, in_total) + col * in_width
        if out_halo:
            lane_out = local_of(lane_out, out_width, out_total)
        j = lane_out + col * out_width
        if expanding:
            w = expand_tap(2 * g - j)
            w = w + jnp.where(g >= 1, expand_tap(-2 * g - j), 0.0)
            w = w + expand_tap(2 * (2 * in_cols - 1 - g) - j)
        else:
            w = reduce_tap(g - 2 * j)
            w = w + jnp.where(g >= 1, reduce_tap(-g - 2 * j), 0.0)
            w = w + jnp.where(g <= in_cols - 2, reduce_tap(2 * (in_cols - 1) - g - 2 * j), 0.0)
        w = jnp.where((g >= 0) & (g < in_cols), w, 0.0)
        ref[pl.ds(pl.multiple_of(base, chunk), chunk), :] = w.astype(BF16)
        return carry

    lax.fori_loop(0, in_total // chunk, one, 0)


def product(values, weights):
    high = values.astype(BF16)
    rest = values - high.astype(F32)
    middle = rest.astype(BF16)
    low = (rest - middle.astype(F32)).astype(BF16)
    out = jnp.dot(low, weights, preferred_element_type=F32)
    out = out + jnp.dot(middle, weights, preferred_element_type=F32)
    return out + jnp.dot(high, weights, preferred_element_type=F32)


def strided(ref, channel, start, count):
    tiles = ref.shape[1]
    return [ref[channel, t, pl.ds(start, count, stride=2), :] for t in range(tiles)]


def kernel(
    image_cols, x_hbm, d0_hbm, d1_ref, d2_ref, d3_ref, d4_ref, c_ref,
    x, send_l, send_r, got_l, got_r, corner,
    v1, l1, l2own, l2, l2side, v3, l3, v4, l4, v5, l5, exp_buf, d0,
    w1, w2, w3, w4, w5, e1, e2, e3, e4, e5,
    local_sem, send_a, recv_a, send_b, recv_b,
):
    channels, rows, width = x_hbm.shape
    row, col = lax.axis_index("rows"), lax.axis_index("cols")
    last_row, last_col = lax.axis_size("rows") - 1, lax.axis_size("cols") - 1
    top, bottom, left, right = row == 0, row == last_row, col == 0, col == last_col
    tiles = width // LANES

    def exists(direction):
        dr, dc = direction
        ok = None
        for flag in ([top] if dr < 0 else [bottom] if dr > 0 else []) + ([left] if dc < 0 else [right] if dc > 0 else []):
            ok = jnp.logical_not(flag) if ok is None else jnp.logical_and(ok, jnp.logical_not(flag))
        return ok

    takes = [
        pltpu.make_async_copy(
            x_hbm.at[:, :, pl.ds(t * LANES, LANES)], x.at[:, t, pl.ds(EDGE, rows), :], local_sem.at[t]
        )
        for t in range(tiles)
    ]
    for take in takes:
        take.start()

    barrier = pltpu.get_barrier_semaphore()
    for direction in DIRECTIONS:
        @pl.when(exists(direction))
        def _(direction=direction):
            pl.semaphore_signal(
                barrier, inc=1, device_id=(row + direction[0], col + direction[1]), device_id_type=MESH
            )

    widths = [width >> k for k in range(LEVELS + 1)]
    cols = [image_cols >> k for k in range(LEVELS + 1)]
    fill_weights(w1, col, widths[0], cols[0], widths[1], True, False)

    for take in takes:
        take.wait()
    for ch in range(channels):
        send_l[ch] = x[ch, 0, pl.ds(EDGE, rows), :].T[:EDGE]
        send_r[ch] = x[ch, tiles - 1, pl.ds(EDGE, rows), :].T[LANES - EDGE:]

    tall = 3 - jnp.where(top, 1, 0) - jnp.where(bottom, 1, 0)
    broad = 3 - jnp.where(left, 1, 0) - jnp.where(right, 1, 0)
    pl.semaphore_wait(barrier, tall * broad - 1)

    def copy_a(number):
        dr, dc = DIRECTIONS[number]
        if dc == 0:
            src = x.at[:, pl.ds(0, tiles), pl.ds(EDGE, EDGE) if dr < 0 else pl.ds(rows, EDGE), :]
            dst = x.at[:, pl.ds(0, tiles), pl.ds(rows + EDGE, EDGE) if dr < 0 else pl.ds(0, EDGE), :]
        elif dr == 0:
            src, dst = (send_l, got_r) if dc < 0 else (send_r, got_l)
        else:
            src = x.at[:, 0 if dc < 0 else tiles - 1, pl.ds(EDGE, EDGE) if dr < 0 else pl.ds(rows, EDGE), :]
            dst = corner.at[number - 4]
        return pltpu.make_async_remote_copy(
            src_ref=src, dst_ref=dst, send_sem=send_a.at[number], recv_sem=recv_a.at[number],
            device_id=(row + dr, col + dc), device_id_type=MESH,
        )

    rows2 = rows // 4

    def copy_b(number):
        dr, dc = DIRECTIONS[number]
        if dr < 0:
            src_rows, dst_rows = pl.ds(0, BELOW), pl.ds(ABOVE + rows2, BELOW)
        elif dr > 0:
            src_rows, dst_rows = pl.ds(rows2 - ABOVE, ABOVE), pl.ds(0, ABOVE)
        else:
            src_rows, dst_rows = pl.ds(0, rows2), pl.ds(ABOVE, rows2)
        dst = l2.at[:, 0, dst_rows, :] if dc == 0 else l2side.at[0 if dc > 0 else 1, :, dst_rows, :]
        return pltpu.make_async_remote_copy(
            src_ref=l2own.at[:, src_rows, :], dst_ref=dst, send_sem=send_b.at[number], recv_sem=recv_b.at[number],
            device_id=(row + dr, col + dc), device_id_type=MESH,
        )

    def each(copy, opposite, act):
        for number, (dr, dc) in enumerate(DIRECTIONS):
            @pl.when(exists((-dr, -dc) if opposite else (dr, dc)))
            def _(number=number):
                act(copy(number))

    each(copy_a, False, lambda c: c.start())
    fill_weights(w2, col, widths[1], cols[1], widths[2], False, False)
    fill_weights(e1, col, widths[1], cols[1], widths[0], False, True)
    each(copy_a, True, lambda c: c.wait_recv())

    lane = lax.broadcasted_iota(jnp.int32, (EDGE, LANES), 1)
    on_right = lane < LANES // 2
    for ch in range(channels):
        gap = jnp.zeros((LANES - 2 * EDGE, rows), F32)
        from_right = jnp.where(right, 0.0, got_r[ch])
        from_left = jnp.where(left, 0.0, got_l[ch])
        x[ch, tiles, pl.ds(EDGE, rows), :] = jnp.concatenate([from_right, gap, from_left], axis=0).T
        for above in (True, False):
            low = corner[3 if above else 1, ch]
            high = corner[2 if above else 0, ch]
            mixed = jnp.where(on_right, jnp.where(right, 0.0, high), jnp.where(left, 0.0, low))
            x[ch, tiles, pl.ds(0 if above else rows + EDGE, EDGE), :] = mixed

    def at_ends(ref, first, own, reducing):
        lead = (slice(None),) * (len(ref.shape) - 2)

        @pl.when(top)
        def _():
            ref[lead + (pl.ds(first - 1, 1),)] = ref[lead + (pl.ds(first + 1, 1),)]
            if reducing:
                ref[lead + (pl.ds(first - 2, 1),)] = ref[lead + (pl.ds(first + 2, 1),)]

        @pl.when(bottom)
        def _():
            ref[lead + (pl.ds(first + own, 1),)] = ref[lead + (pl.ds(first + own - (2 if reducing else 1), 1),)]

    def reduce_rows(src, dst, start, count):
        for ch in range(channels):
            for t in range(src.shape[1]):
                part = [src[ch, t, pl.ds(start + k, count, stride=2), :] for k in range(5)]
                total = (part[0] + part[4]) * 0.0625 + (part[1] + part[3]) * 0.25 + part[2] * 0.375
                dst[ch, pl.ds(0, count), pl.ds(t * LANES, LANES)] = total

    def reduce_cols(src, weights, dst):
        depth = src.shape[1]
        out = product(src[...].reshape(channels * depth, src.shape[2]), weights[...])
        for ch in range(channels):
            for t in range(dst.shape[1]):
                dst[ch, t] = out[ch * depth:(ch + 1) * depth, t * LANES:(t + 1) * LANES]

    def residual(fine, fine_first, coarse, first, own, weights, out, out_width):
        at_ends(coarse, first, own, False)
        depth = coarse.shape[2]
        flat = jnp.concatenate(
            [coarse[:, t].reshape(channels * depth, LANES) for t in range(coarse.shape[1])], axis=1
        )
        wide = product(flat, weights[...])
        out_tiles = weights.shape[1] // LANES
        for t in range(out_tiles):
            exp_buf[pl.ds(0, channels * depth), :] = wide[:, t * LANES:(t + 1) * LANES]
            for ch in range(channels):
                at = ch * depth + first
                before = exp_buf[pl.ds(at - 1, own), :]
                center = exp_buf[pl.ds(at, own), :]
                after = exp_buf[pl.ds(at + 1, own), :]
                even = fine[ch, t, pl.ds(fine_first, own, stride=2), :] - (before + 6.0 * center + after) * 0.125
                odd = fine[ch, t, pl.ds(fine_first + 1, own, stride=2), :] - (center + after) * 0.5
                d0[ch, t, pl.ds(0, own, stride=2), :] = even
                d0[ch, t, pl.ds(1, own, stride=2), :] = odd
        if out is not None:
            for ch in range(channels):
                for t in range(out_tiles):
                    lanes = min(LANES, out_width)
                    out[ch, :, pl.ds(t * LANES, lanes)] = d0[ch, t, pl.ds(0, 2 * own), :][:, :lanes]

    at_ends(x, EDGE, rows, True)
    first1 = (EDGE - 2) // 2
    count1 = (x.shape[2] - 3 - EDGE) // 2 + first1 + 1
    reduce_rows(x, v1, EDGE - 2 - 2 * first1, count1)
    reduce_cols(v1, w1, l1)
    at_ends(l1, first1, rows // 2, True)
    reduce_rows(l1, v5, first1 - 2, rows2)
    own = product(
        v5[:, pl.ds(0, rows2), :].reshape(channels * rows2, v5.shape[2]), w2[...]
    )
    for ch in range(channels):
        l2own[ch] = own[ch * rows2:(ch + 1) * rows2]
        l2[ch, 0, pl.ds(ABOVE, rows2), :] = own[ch * rows2:(ch + 1) * rows2]
    each(copy_b, False, lambda c: c.start())

    residual(x, EDGE, l1, first1, rows // 2, e1, None, width)
    puts = [
        pltpu.make_async_copy(d0.at[:, t], d0_hbm.at[:, :, pl.ds(t * LANES, LANES)], local_sem.at[t])
        for t in range(tiles)
    ]
    for put in puts:
        put.start()
    fill_weights(w3, col, widths[2], cols[2], widths[3], True, False)
    fill_weights(e2, col, widths[2], cols[2], widths[1], False, True)
    fill_weights(w4, col, widths[3], cols[3], widths[4], True, False)
    fill_weights(w5, col, widths[4], cols[4], widths[5], True, False)
    fill_weights(e3, col, widths[3], cols[3], widths[2], False, True)
    fill_weights(e4, col, widths[4], cols[4], widths[3], False, True)
    fill_weights(e5, col, widths[5], cols[5], widths[4], False, True)
    each(copy_b, True, lambda c: c.wait_recv())

    lane = lax.broadcasted_iota(jnp.int32, (l2.shape[2], LANES), 1)
    for ch in range(channels):
        l2[ch, 1] = jnp.where(
            lane < LANES // 2,
            jnp.where(right, 0.0, l2side[1, ch]),
            jnp.where(left, 0.0, l2side[0, ch]),
        )

    for put in puts:
        put.wait()

    firsts = [EDGE, first1, ABOVE]
    counts = [None, None, l2.shape[2]]
    residual(l1, first1, l2, ABOVE, rows2, e2, d1_ref, widths[1])
    level, fine = l2, l2
    owns = [rows >> k for k in range(LEVELS + 1)]
    stages = ((v3, w3, l3, e3, d2_ref), (v4, w4, l4, e4, d3_ref), (None, w5, l5, e5, d4_ref))
    for k, (v, w, coarse, e, out) in enumerate(stages, start=2):
        if v is None:
            v = v4
        at_ends(level, firsts[k], owns[k], True)
        first = (firsts[k] - 2) // 2
        count = (counts[k] - 3 - firsts[k]) // 2 + first + 1
        depth = -(-count // 8) * 8
        firsts.append(first)
        counts.append(count)
        for ch in range(channels):
            for t in range(level.shape[1]):
                part = [level[ch, t, pl.ds(firsts[k] - 2 - 2 * first + i, count, stride=2), :] for i in range(5)]
                total = (part[0] + part[4]) * 0.0625 + (part[1] + part[3]) * 0.25 + part[2] * 0.375
                v[ch, pl.ds(0, count), pl.ds(t * LANES, LANES)] = total
        made = product(v[:, pl.ds(0, depth), :].reshape(channels * depth, v.shape[2]), w[...])
        for ch in range(channels):
            coarse[ch, 0] = made[ch * depth:(ch + 1) * depth]
        residual(level, firsts[k], coarse, first, owns[k + 1], e, out, widths[k])
        level = coarse
    for ch in range(channels):
        c_ref[ch] = l5[ch, 0, pl.ds(firsts[5], owns[5]), :][:, :widths[5]]

    each(copy_a, False, lambda c: c.wait_send())
    each(copy_b, False, lambda c: c.wait_send())


def solution(mesh):
    def body(x):
        channels, rows, width = x.shape
        image_cols = width * mesh.shape["cols"]
        widths = [width >> k for k in range(LEVELS + 1)]
        p = [pitch(w) for w in widths]
        vm = lambda *shape: pltpu.VMEM(shape, F32)
        wt = lambda *shape: pltpu.VMEM(shape, BF16)
        rows2 = rows // 4
        ext = ABOVE + rows2 + BELOW
        up8 = lambda n: -(-n // 8) * 8
        n1 = up8(rows // 2 + EDGE - 2)
        f3, n3 = (ABOVE - 2) // 2, (ext - 3 - ABOVE) // 2 + (ABOVE - 2) // 2 + 1
        f4, n4 = (f3 - 2) // 2, (n3 - 3 - f3) // 2 + (f3 - 2) // 2 + 1
        n5 = (n4 - 3 - f4) // 2 + (f4 - 2) // 2 + 1
        shape = lambda k: jax.ShapeDtypeStruct((channels, rows >> k, width >> k), F32)
        vmem = pl.BlockSpec(memory_space=pltpu.VMEM)
        anywhere = pl.BlockSpec(memory_space=pl.ANY)
        return pl.pallas_call(
            functools.partial(kernel, image_cols),
            out_shape=tuple(shape(k) for k in range(LEVELS + 1)),
            in_specs=[anywhere],
            out_specs=(anywhere,) + (vmem,) * LEVELS,
            scratch_shapes=[
                vm(channels, p[0] // LANES, rows + 2 * EDGE, LANES),
                vm(channels, EDGE, rows), vm(channels, EDGE, rows),
                vm(channels, EDGE, rows), vm(channels, EDGE, rows),
                vm(4, channels, EDGE, LANES),
                vm(channels, n1, p[0]),
                vm(channels, p[1] // LANES, n1, LANES),
                vm(channels, rows2, LANES),
                vm(channels, p[2] // LANES, ext, LANES),
                vm(2, channels, ext, LANES),
                vm(channels, up8(n3), p[2]),
                vm(channels, 1, up8(n3), LANES),
                vm(channels, up8(n4), p[3]),
                vm(channels, 1, up8(n4), LANES),
                vm(channels, rows2, p[1]),
                vm(channels, 1, up8(n5), LANES),
                vm(channels * max(n1, ext) + 8, LANES),
                vm(channels, width // LANES, rows, LANES),
                wt(p[0], p[1]), wt(p[1], widths[2]), wt(p[2], p[3]), wt(p[3], p[4]), wt(p[4], p[5]),
                wt(p[1], widths[0]), wt(p[2], widths[1]), wt(p[3], LANES), wt(p[4], LANES), wt(p[5], LANES),
                pltpu.SemaphoreType.DMA((width // LANES,)),
                pltpu.SemaphoreType.DMA((8,)), pltpu.SemaphoreType.DMA((8,)),
                pltpu.SemaphoreType.DMA((8,)), pltpu.SemaphoreType.DMA((8,)),
            ],
            compiler_params=pltpu.CompilerParams(collective_id=0, has_side_effects=True),
            name="pyramid",
        )(x)

    placed = P(None, "rows", "cols")
    return jax.shard_map(
        body, mesh=mesh, in_specs=(placed,), out_specs=(placed,) * (LEVELS + 1), check_vma=False
    )
```

```python
import functools

import jax
import jax.numpy as jnp
from jax import lax
from jax.experimental import pallas as pl
from jax.experimental.pallas import tpu as pltpu
from jax.sharding import PartitionSpec as P

LEVELS = 5
LANES = 128
EDGE = 8
ABOVE, BELOW = 24, 16
VMEM_GRANT = 24 << 20
BF16 = jnp.bfloat16
F32 = jnp.float32
MESH = pl.DeviceIdType.MESH
DIRECTIONS = ((-1, 0), (1, 0), (0, -1), (0, 1), (-1, -1), (-1, 1), (1, -1), (1, 1))


def pitch(width):
    return width + LANES if width >= LANES else LANES


def local_of(lane, width, total):
    return jnp.where(lane < width + (total - width) // 2, lane, lane - total)


def reduce_tap(distance):
    far = jnp.abs(distance)
    return jnp.where(far == 0, 0.375, jnp.where(far == 1, 0.25, jnp.where(far == 2, 0.0625, 0.0)))


def expand_tap(distance):
    far = jnp.abs(distance)
    return jnp.where(far == 0, 0.75, jnp.where(far == 1, 0.5, jnp.where(far == 2, 0.125, 0.0)))


def fill_weights(ref, col, in_width, in_cols, out_width, out_halo, expanding):
    in_total, out_total = ref.shape
    chunk = 32

    def one(step, carry):
        base = step * chunk
        lane_in = base + lax.broadcasted_iota(jnp.int32, (chunk, out_total), 0)
        lane_out = lax.broadcasted_iota(jnp.int32, (chunk, out_total), 1)
        g = local_of(lane_in, in_width, in_total) + col * in_width
        if out_halo:
            lane_out = local_of(lane_out, out_width, out_total)
        j = lane_out + col * out_width
        if expanding:
            w = expand_tap(2 * g - j)
            w = w + jnp.where(g >= 1, expand_tap(-2 * g - j), 0.0)
            w = w + expand_tap(2 * (2 * in_cols - 1 - g) - j)
        else:
            w = reduce_tap(g - 2 * j)
            w = w + jnp.where(g >= 1, reduce_tap(-g - 2 * j), 0.0)
            w = w + jnp.where(g <= in_cols - 2, reduce_tap(2 * (in_cols - 1) - g - 2 * j), 0.0)
        w = jnp.where((g >= 0) & (g < in_cols), w, 0.0)
        ref[pl.ds(pl.multiple_of(base, chunk), chunk), :] = w.astype(BF16)
        return carry

    lax.fori_loop(0, in_total // chunk, one, 0)


def product(values, weights):
    high = values.astype(BF16)
    rest = values - high.astype(F32)
    middle = rest.astype(BF16)
    low = (rest - middle.astype(F32)).astype(BF16)
    out = jnp.dot(low, weights, preferred_element_type=F32)
    out = out + jnp.dot(middle, weights, preferred_element_type=F32)
    return out + jnp.dot(high, weights, preferred_element_type=F32)


def hand_out(first5, d0, d1, d2, d3, d4, l5, d0_hbm, d1_hbm, d2_hbm, d3_out, d4_out, c_out, sem):
    puts = []
    for src, dst in ((d0, d0_hbm), (d1, d1_hbm), (d2, d2_hbm)):
        for t in range(src.shape[1]):
            puts.append(
                pltpu.make_async_copy(src.at[:, t], dst.at[:, :, pl.ds(t * LANES, LANES)], sem.at[len(puts)])
            )
    for put in puts:
        put.start()
    for ch in range(d3_out.shape[0]):
        d3_out[ch] = d3[ch, 0][:, :d3_out.shape[2]]
        d4_out[ch] = d4[ch, 0][:, :d4_out.shape[2]]
        c_out[ch] = l5[ch, 0, pl.ds(first5, c_out.shape[1]), :][:, :c_out.shape[2]]
    for put in puts:
        put.wait()


def kernel(
    image_cols, x_hbm, d0, d1, d2, d3, d4, l5,
    x, send_l, send_r, got_l, got_r, corner,
    v1, l1, l2own, l2, l2side, v3, l3, v4, l4, v5, v2, exp0, exp1, exp2, exp3, exp4,
    w1, w2, w3, w4, w5, e1, e2, e3, e4, e5,
    local_sem, send_a, recv_a, send_b, recv_b,
):
    channels, rows, width = x_hbm.shape
    row, col = lax.axis_index("rows"), lax.axis_index("cols")
    last_row, last_col = lax.axis_size("rows") - 1, lax.axis_size("cols") - 1
    top, bottom, left, right = row == 0, row == last_row, col == 0, col == last_col
    tiles = width // LANES

    def exists(direction):
        dr, dc = direction
        ok = None
        for flag in ([top] if dr < 0 else [bottom] if dr > 0 else []) + ([left] if dc < 0 else [right] if dc > 0 else []):
            ok = jnp.logical_not(flag) if ok is None else jnp.logical_and(ok, jnp.logical_not(flag))
        return ok

    takes = [
        pltpu.make_async_copy(
            x_hbm.at[:, :, pl.ds(t * LANES, LANES)], x.at[:, t, pl.ds(EDGE, rows), :], local_sem.at[t]
        )
        for t in range(tiles)
    ]
    for take in takes:
        take.start()

    barrier = pltpu.get_barrier_semaphore()
    for direction in DIRECTIONS:
        @pl.when(exists(direction))
        def _(direction=direction):
            pl.semaphore_signal(
                barrier, inc=1, device_id=(row + direction[0], col + direction[1]), device_id_type=MESH
            )

    widths = [width >> k for k in range(LEVELS + 1)]
    cols = [image_cols >> k for k in range(LEVELS + 1)]
    fill_weights(w1, col, widths[0], cols[0], widths[1], True, False)

    for take in takes:
        take.wait()
    for ch in range(channels):
        send_l[ch] = x[ch, 0, pl.ds(EDGE, rows), :].T[:EDGE]
        send_r[ch] = x[ch, tiles - 1, pl.ds(EDGE, rows), :].T[LANES - EDGE:]

    tall = 3 - jnp.where(top, 1, 0) - jnp.where(bottom, 1, 0)
    broad = 3 - jnp.where(left, 1, 0) - jnp.where(right, 1, 0)
    pl.semaphore_wait(barrier, tall * broad - 1)

    def copy_a(number):
        dr, dc = DIRECTIONS[number]
        if dc == 0:
            src = x.at[:, pl.ds(0, tiles), pl.ds(EDGE, EDGE) if dr < 0 else pl.ds(rows, EDGE), :]
            dst = x.at[:, pl.ds(0, tiles), pl.ds(rows + EDGE, EDGE) if dr < 0 else pl.ds(0, EDGE), :]
        elif dr == 0:
            src, dst = (send_l, got_r) if dc < 0 else (send_r, got_l)
        else:
            src = x.at[:, 0 if dc < 0 else tiles - 1, pl.ds(EDGE, EDGE) if dr < 0 else pl.ds(rows, EDGE), :]
            dst = corner.at[number - 4]
        return pltpu.make_async_remote_copy(
            src_ref=src, dst_ref=dst, send_sem=send_a.at[number], recv_sem=recv_a.at[number],
            device_id=(row + dr, col + dc), device_id_type=MESH,
        )

    rows2 = rows // 4

    def copy_b(number):
        dr, dc = DIRECTIONS[number]
        if dr < 0:
            src_rows, dst_rows = pl.ds(0, BELOW), pl.ds(ABOVE + rows2, BELOW)
        elif dr > 0:
            src_rows, dst_rows = pl.ds(rows2 - ABOVE, ABOVE), pl.ds(0, ABOVE)
        else:
            src_rows, dst_rows = pl.ds(0, rows2), pl.ds(ABOVE, rows2)
        dst = l2.at[:, 0, dst_rows, :] if dc == 0 else l2side.at[0 if dc > 0 else 1, :, dst_rows, :]
        return pltpu.make_async_remote_copy(
            src_ref=l2own.at[:, src_rows, :], dst_ref=dst, send_sem=send_b.at[number], recv_sem=recv_b.at[number],
            device_id=(row + dr, col + dc), device_id_type=MESH,
        )

    def each(copy, opposite, act):
        for number, (dr, dc) in enumerate(DIRECTIONS):
            @pl.when(exists((-dr, -dc) if opposite else (dr, dc)))
            def _(number=number):
                act(copy(number))

    each(copy_a, False, lambda c: c.start())
    fill_weights(w2, col, widths[1], cols[1], widths[2], False, False)
    fill_weights(e1, col, widths[1], cols[1], widths[0], False, True)
    each(copy_a, True, lambda c: c.wait_recv())

    lane = lax.broadcasted_iota(jnp.int32, (EDGE, LANES), 1)
    on_right = lane < LANES // 2
    for ch in range(channels):
        gap = jnp.zeros((LANES - 2 * EDGE, rows), F32)
        from_right = jnp.where(right, 0.0, got_r[ch])
        from_left = jnp.where(left, 0.0, got_l[ch])
        x[ch, tiles, pl.ds(EDGE, rows), :] = jnp.concatenate([from_right, gap, from_left], axis=0).T
        for above in (True, False):
            low = corner[3 if above else 1, ch]
            high = corner[2 if above else 0, ch]
            mixed = jnp.where(on_right, jnp.where(right, 0.0, high), jnp.where(left, 0.0, low))
            x[ch, tiles, pl.ds(0 if above else rows + EDGE, EDGE), :] = mixed

    def at_ends(ref, first, own, reducing):
        lead = (slice(None),) * (len(ref.shape) - 2)

        def fix(flag, to, source):
            to, source = lead + (pl.ds(to, 1),), lead + (pl.ds(source, 1),)
            ref[to] = jnp.where(flag, ref[source], ref[to])

        fix(top, first - 1, first + 1)
        if reducing:
            fix(top, first - 2, first + 2)
        fix(bottom, first + own, first + own - (2 if reducing else 1))

    def reduce_rows(src, dst, start, count):
        for ch in range(channels):
            for t in range(src.shape[1]):
                part = [src[ch, t, pl.ds(start + k, count, stride=2), :] for k in range(5)]
                total = (part[0] + part[4]) * 0.0625 + (part[1] + part[3]) * 0.25 + part[2] * 0.375
                dst[ch, pl.ds(0, count), pl.ds(t * LANES, LANES)] = total

    def reduce_cols(src, weights, dst):
        depth = src.shape[1]
        out = product(src[...].reshape(channels * depth, src.shape[2]), weights[...])
        for ch in range(channels):
            for t in range(dst.shape[1]):
                dst[ch, t] = out[ch * depth:(ch + 1) * depth, t * LANES:(t + 1) * LANES]

    def residual(fine, fine_first, coarse, first, own, weights, buffer, out):
        at_ends(coarse, first, own, False)
        depth = coarse.shape[2]
        flat = jnp.concatenate(
            [coarse[:, t].reshape(channels * depth, LANES) for t in range(coarse.shape[1])], axis=1
        )
        wide = product(flat, weights[...])
        for t in range(out.shape[1]):
            buffer[t] = wide[:, t * LANES:(t + 1) * LANES]
            for ch in range(channels):
                at = ch * depth + first
                before = buffer[t, pl.ds(at - 1, own), :]
                center = buffer[t, pl.ds(at, own), :]
                after = buffer[t, pl.ds(at + 1, own), :]
                even = fine[ch, t, pl.ds(fine_first, own, stride=2), :] - (before + 6.0 * center + after) * 0.125
                odd = fine[ch, t, pl.ds(fine_first + 1, own, stride=2), :] - (center + after) * 0.5
                out[ch, t, pl.ds(0, own, stride=2), :] = even
                out[ch, t, pl.ds(1, own, stride=2), :] = odd

    at_ends(x, EDGE, rows, True)
    first1 = (EDGE - 2) // 2
    count1 = (x.shape[2] - 3 - EDGE) // 2 + first1 + 1
    reduce_rows(x, v1, EDGE - 2 - 2 * first1, count1)
    reduce_cols(v1, w1, l1)
    at_ends(l1, first1, rows // 2, True)
    reduce_rows(l1, v2, first1 - 2, rows2)
    own = product(
        v2[...].reshape(channels * rows2, v2.shape[2]), w2[...]
    )
    for ch in range(channels):
        l2own[ch] = own[ch * rows2:(ch + 1) * rows2]
        l2[ch, 0, pl.ds(ABOVE, rows2), :] = own[ch * rows2:(ch + 1) * rows2]
    each(copy_b, False, lambda c: c.start())

    residual(x, EDGE, l1, first1, rows // 2, e1, exp0, d0)
    fill_weights(w3, col, widths[2], cols[2], widths[3], True, False)
    fill_weights(e2, col, widths[2], cols[2], widths[1], False, True)
    fill_weights(w4, col, widths[3], cols[3], widths[4], True, False)
    fill_weights(w5, col, widths[4], cols[4], widths[5], True, False)
    fill_weights(e3, col, widths[3], cols[3], widths[2], False, True)
    fill_weights(e4, col, widths[4], cols[4], widths[3], False, True)
    fill_weights(e5, col, widths[5], cols[5], widths[4], False, True)
    each(copy_b, True, lambda c: c.wait_recv())

    lane = lax.broadcasted_iota(jnp.int32, (l2.shape[2], LANES), 1)
    for ch in range(channels):
        l2[ch, 1] = jnp.where(
            lane < LANES // 2,
            jnp.where(right, 0.0, l2side[1, ch]),
            jnp.where(left, 0.0, l2side[0, ch]),
        )

    firsts = [EDGE, first1, ABOVE]
    counts = [None, None, l2.shape[2]]
    residual(l1, first1, l2, ABOVE, rows2, e2, exp1, d1)
    level = l2
    owns = [rows >> k for k in range(LEVELS + 1)]
    stages = ((v3, w3, l3, e3, exp2, d2), (v4, w4, l4, e4, exp3, d3), (v5, w5, l5, e5, exp4, d4))
    for k, (v, w, coarse, e, buffer, out) in enumerate(stages, start=2):
        at_ends(level, firsts[k], owns[k], True)
        first = (firsts[k] - 2) // 2
        count = (counts[k] - 3 - firsts[k]) // 2 + first + 1
        depth = -(-count // 8) * 8
        firsts.append(first)
        counts.append(count)
        for ch in range(channels):
            for t in range(level.shape[1]):
                part = [level[ch, t, pl.ds(firsts[k] - 2 - 2 * first + i, count, stride=2), :] for i in range(5)]
                total = (part[0] + part[4]) * 0.0625 + (part[1] + part[3]) * 0.25 + part[2] * 0.375
                v[ch, pl.ds(0, count), pl.ds(t * LANES, LANES)] = total
        made = product(v[:, pl.ds(0, depth), :].reshape(channels * depth, v.shape[2]), w[...])
        for ch in range(channels):
            coarse[ch, 0] = made[ch * depth:(ch + 1) * depth]
        residual(level, firsts[k], coarse, first, owns[k + 1], e, buffer, out)
        level = coarse
    each(copy_a, False, lambda c: c.wait_send())
    each(copy_b, False, lambda c: c.wait_send())


def solution(mesh):
    def body(x):
        channels, rows, width = x.shape
        image_cols = width * mesh.shape["cols"]
        widths = [width >> k for k in range(LEVELS + 1)]
        p = [pitch(w) for w in widths]
        vm = lambda *shape: pltpu.VMEM(shape, F32)
        wt = lambda *shape: pltpu.VMEM(shape, BF16)
        rows2 = rows // 4
        ext = ABOVE + rows2 + BELOW
        up8 = lambda n: -(-n // 8) * 8
        n1 = up8(rows // 2 + EDGE - 2)
        f3, n3 = (ABOVE - 2) // 2, (ext - 3 - ABOVE) // 2 + (ABOVE - 2) // 2 + 1
        f4, n4 = (f3 - 2) // 2, (n3 - 3 - f3) // 2 + (f3 - 2) // 2 + 1
        n5 = (n4 - 3 - f4) // 2 + (f4 - 2) // 2 + 1
        f5 = (f4 - 2) // 2
        shape = lambda k: jax.ShapeDtypeStruct((channels, rows >> k, width >> k), F32)
        tiled = [(channels, max(widths[k] // LANES, 1), rows >> k, LANES) for k in range(LEVELS)]
        tiled.append((channels, 1, up8(n5), LANES))
        depths = [n1, ext, up8(n3), up8(n4), up8(n5)]
        vmem = pl.BlockSpec(memory_space=pltpu.VMEM)
        anywhere = pl.BlockSpec(memory_space=pl.ANY)
        held = pl.pallas_call(
            functools.partial(kernel, image_cols),
            out_shape=tuple(vm(*dims) for dims in tiled),
            in_specs=[anywhere],
            out_specs=(vmem,) * (LEVELS + 1),
            scratch_shapes=[
                vm(channels, p[0] // LANES, rows + 2 * EDGE, LANES),
                vm(channels, EDGE, rows), vm(channels, EDGE, rows),
                vm(channels, EDGE, rows), vm(channels, EDGE, rows),
                vm(4, channels, EDGE, LANES),
                vm(channels, n1, p[0]),
                vm(channels, p[1] // LANES, n1, LANES),
                vm(channels, rows2, LANES),
                vm(channels, p[2] // LANES, ext, LANES),
                vm(2, channels, ext, LANES),
                vm(channels, up8(n3), p[2]),
                vm(channels, 1, up8(n3), LANES),
                vm(channels, up8(n4), p[3]),
                vm(channels, 1, up8(n4), LANES),
                vm(channels, up8(n5), p[4]),
                vm(channels, rows2, p[1]),
                *(vm(tiled[k][1], channels * depths[k], LANES) for k in range(LEVELS)),
                wt(p[0], p[1]), wt(p[1], widths[2]), wt(p[2], p[3]), wt(p[3], p[4]), wt(p[4], p[5]),
                wt(p[1], widths[0]), wt(p[2], widths[1]), wt(p[3], LANES), wt(p[4], LANES), wt(p[5], LANES),
                pltpu.SemaphoreType.DMA((width // LANES,)),
                pltpu.SemaphoreType.DMA((8,)), pltpu.SemaphoreType.DMA((8,)),
                pltpu.SemaphoreType.DMA((8,)), pltpu.SemaphoreType.DMA((8,)),
            ],
            compiler_params=pltpu.CompilerParams(
                collective_id=0, has_side_effects=True, vmem_limit_bytes=VMEM_GRANT
            ),
            name="pyramid",
        )(x)
        copies = sum(dims[1] for dims in tiled[:3])
        return pl.pallas_call(
            functools.partial(hand_out, f5),
            out_shape=tuple(shape(k) for k in range(LEVELS + 1)),
            in_specs=[anywhere] * 3 + [vmem] * 3,
            out_specs=(anywhere,) * 3 + (vmem,) * 3,
            scratch_shapes=[pltpu.SemaphoreType.DMA((copies,))],
            compiler_params=pltpu.CompilerParams(vmem_limit_bytes=VMEM_GRANT),
            name="hand_out",
        )(*(pltpu.with_memory_space_constraint(part, pltpu.VMEM) for part in held))

    placed = P(None, "rows", "cols")
    return jax.shard_map(
        body, mesh=mesh, in_specs=(placed,), out_specs=(placed,) * (LEVELS + 1), check_vma=False
    )
```

```python
import functools

import jax
import jax.numpy as jnp
from jax import lax
from jax.experimental import pallas as pl
from jax.experimental.pallas import tpu as pltpu
from jax.sharding import PartitionSpec as P

LEVELS = 5
LANES = 128
EDGE = 8
ABOVE, BELOW = 24, 16
VMEM_GRANT = 24 << 20
BF16 = jnp.bfloat16
F32 = jnp.float32
MESH = pl.DeviceIdType.MESH
DIRECTIONS = ((-1, 0), (1, 0), (0, -1), (0, 1), (-1, -1), (-1, 1), (1, -1), (1, 1))


def pitch(width):
    return width + LANES if width >= LANES else LANES


def local_of(lane, width, total):
    return jnp.where(lane < width + (total - width) // 2, lane, lane - total)


def reduce_tap(distance):
    far = jnp.abs(distance)
    return jnp.where(far == 0, 0.375, jnp.where(far == 1, 0.25, jnp.where(far == 2, 0.0625, 0.0)))


def expand_tap(distance):
    far = jnp.abs(distance)
    return jnp.where(far == 0, 0.75, jnp.where(far == 1, 0.5, jnp.where(far == 2, 0.125, 0.0)))


def fill_weights(ref, col, in_width, in_cols, out_width, out_halo, expanding):
    in_total, out_total = ref.shape
    chunk = 32

    def one(step, carry):
        base = step * chunk
        lane_in = base + lax.broadcasted_iota(jnp.int32, (chunk, out_total), 0)
        lane_out = lax.broadcasted_iota(jnp.int32, (chunk, out_total), 1)
        g = local_of(lane_in, in_width, in_total) + col * in_width
        if out_halo:
            lane_out = local_of(lane_out, out_width, out_total)
        j = lane_out + col * out_width
        if expanding:
            w = expand_tap(2 * g - j)
            w = w + jnp.where(g >= 1, expand_tap(-2 * g - j), 0.0)
            w = w + expand_tap(2 * (2 * in_cols - 1 - g) - j)
        else:
            w = reduce_tap(g - 2 * j)
            w = w + jnp.where(g >= 1, reduce_tap(-g - 2 * j), 0.0)
            w = w + jnp.where(g <= in_cols - 2, reduce_tap(2 * (in_cols - 1) - g - 2 * j), 0.0)
        w = jnp.where((g >= 0) & (g < in_cols), w, 0.0)
        ref[pl.ds(pl.multiple_of(base, chunk), chunk), :] = w.astype(BF16)
        return carry

    lax.fori_loop(0, in_total // chunk, one, 0)


def product(values, weights):
    high = values.astype(BF16)
    rest = values - high.astype(F32)
    middle = rest.astype(BF16)
    low = (rest - middle.astype(F32)).astype(BF16)
    out = jnp.dot(low, weights, preferred_element_type=F32)
    out = out + jnp.dot(middle, weights, preferred_element_type=F32)
    return out + jnp.dot(high, weights, preferred_element_type=F32)


def hand_out(first5, d0, d1, d2, d3, d4, l5, d0_hbm, d1_hbm, d2_hbm, d3_out, d4_out, c_out, sem):
    puts = []
    for src, dst in ((d0, d0_hbm), (d1, d1_hbm), (d2, d2_hbm)):
        for t in range(src.shape[1]):
            puts.append(
                pltpu.make_async_copy(src.at[:, t], dst.at[:, :, pl.ds(t * LANES, LANES)], sem.at[len(puts)])
            )
    for put in puts:
        put.start()
    for ch in range(d3_out.shape[0]):
        d3_out[ch] = d3[ch, 0][:, :d3_out.shape[2]]
        d4_out[ch] = d4[ch, 0][:, :d4_out.shape[2]]
        c_out[ch] = l5[ch, 0, pl.ds(first5, c_out.shape[1]), :][:, :c_out.shape[2]]
    for put in puts:
        put.wait()


def kernel(
    image_cols, x_hbm, d0, d1, d2, d3, d4, l5,
    x, send_l, send_r, got_l, got_r, corner,
    v1, l1, l2own, l2, side_l, side_r, side_got_l, side_got_r, v3, l3, v4, l4, v5, v2, exp0, exp1, exp2, exp3, exp4,
    w1, w2, w3, w4, w5, e1, e2, e3, e4, e5,
    local_sem, send_a, recv_a, send_b, recv_b,
):
    channels, rows, width = x_hbm.shape
    row, col = lax.axis_index("rows"), lax.axis_index("cols")
    last_row, last_col = lax.axis_size("rows") - 1, lax.axis_size("cols") - 1
    top, bottom, left, right = row == 0, row == last_row, col == 0, col == last_col
    tiles = width // LANES

    def exists(direction):
        dr, dc = direction
        ok = None
        for flag in ([top] if dr < 0 else [bottom] if dr > 0 else []) + ([left] if dc < 0 else [right] if dc > 0 else []):
            ok = jnp.logical_not(flag) if ok is None else jnp.logical_and(ok, jnp.logical_not(flag))
        return ok

    takes = [
        pltpu.make_async_copy(
            x_hbm.at[:, :, pl.ds(t * LANES, LANES)], x.at[:, t, pl.ds(EDGE, rows), :], local_sem.at[t]
        )
        for t in range(tiles)
    ]
    for take in takes:
        take.start()

    barrier = pltpu.get_barrier_semaphore()
    for direction in DIRECTIONS:
        @pl.when(exists(direction))
        def _(direction=direction):
            pl.semaphore_signal(
                barrier, inc=1, device_id=(row + direction[0], col + direction[1]), device_id_type=MESH
            )

    widths = [width >> k for k in range(LEVELS + 1)]
    cols = [image_cols >> k for k in range(LEVELS + 1)]
    fill_weights(w1, col, widths[0], cols[0], widths[1], True, False)

    for take in takes:
        take.wait()
    for ch in range(channels):
        send_l[ch] = x[ch, 0, pl.ds(EDGE, rows), :].T[:EDGE]
        send_r[ch] = x[ch, tiles - 1, pl.ds(EDGE, rows), :].T[LANES - EDGE:]

    tall = 3 - jnp.where(top, 1, 0) - jnp.where(bottom, 1, 0)
    broad = 3 - jnp.where(left, 1, 0) - jnp.where(right, 1, 0)
    pl.semaphore_wait(barrier, tall * broad - 1)

    def copy_a(number):
        dr, dc = DIRECTIONS[number]
        if dc == 0:
            src = x.at[:, pl.ds(0, tiles), pl.ds(EDGE, EDGE) if dr < 0 else pl.ds(rows, EDGE), :]
            dst = x.at[:, pl.ds(0, tiles), pl.ds(rows + EDGE, EDGE) if dr < 0 else pl.ds(0, EDGE), :]
        elif dr == 0:
            src, dst = (send_l, got_r) if dc < 0 else (send_r, got_l)
        else:
            src = x.at[:, 0 if dc < 0 else tiles - 1, pl.ds(EDGE, EDGE) if dr < 0 else pl.ds(rows, EDGE), :]
            dst = corner.at[number - 4]
        return pltpu.make_async_remote_copy(
            src_ref=src, dst_ref=dst, send_sem=send_a.at[number], recv_sem=recv_a.at[number],
            device_id=(row + dr, col + dc), device_id_type=MESH,
        )

    rows2 = rows // 4

    def copy_b(number):
        dr, dc = DIRECTIONS[number]
        if dr < 0:
            src_rows, dst_rows = pl.ds(0, BELOW), pl.ds(ABOVE + rows2, BELOW)
        elif dr > 0:
            src_rows, dst_rows = pl.ds(rows2 - ABOVE, ABOVE), pl.ds(0, ABOVE)
        else:
            src_rows, dst_rows = pl.ds(0, rows2), pl.ds(ABOVE, rows2)
        if dc == 0:
            src, dst = l2own.at[:, src_rows, :], l2.at[:, 0, dst_rows, :]
        elif dc < 0:
            src, dst = side_l, side_got_r.at[1 - dr]
        else:
            src, dst = side_r, side_got_l.at[1 - dr]
        return pltpu.make_async_remote_copy(
            src_ref=src, dst_ref=dst, send_sem=send_b.at[number], recv_sem=recv_b.at[number],
            device_id=(row + dr, col + dc), device_id_type=MESH,
        )

    def each(copy, opposite, act):
        for number, (dr, dc) in enumerate(DIRECTIONS):
            @pl.when(exists((-dr, -dc) if opposite else (dr, dc)))
            def _(number=number):
                act(copy(number))

    each(copy_a, False, lambda c: c.start())
    fill_weights(w2, col, widths[1], cols[1], widths[2], False, False)
    fill_weights(e1, col, widths[1], cols[1], widths[0], False, True)
    def at_ends(ref, first, own, reducing):
        lead = (slice(None),) * (len(ref.shape) - 2)

        def fix(flag, to, source):
            to, source = lead + (pl.ds(to, 1),), lead + (pl.ds(source, 1),)
            ref[to] = jnp.where(flag, ref[source], ref[to])

        fix(top, first - 1, first + 1)
        if reducing:
            fix(top, first - 2, first + 2)
        fix(bottom, first + own, first + own - (2 if reducing else 1))

    def reduce_rows(src, dst, start, count, at=0, lane_tiles=None):
        for ch in range(channels):
            for t in range(src.shape[1]) if lane_tiles is None else lane_tiles:
                part = [src[ch, t, pl.ds(start + 2 * at + k, count, stride=2), :] for k in range(5)]
                total = (part[0] + part[4]) * 0.0625 + (part[1] + part[3]) * 0.25 + part[2] * 0.375
                dst[ch, pl.ds(at, count), pl.ds(t * LANES, LANES)] = total

    def residual(fine, fine_first, coarse, first, own, weights, buffer, out):
        at_ends(coarse, first, own, False)
        depth = coarse.shape[2]
        flat = jnp.concatenate(
            [coarse[:, t].reshape(channels * depth, LANES) for t in range(coarse.shape[1])], axis=1
        )
        wide = product(flat, weights[...])
        for t in range(out.shape[1]):
            buffer[t] = wide[:, t * LANES:(t + 1) * LANES]
            for ch in range(channels):
                at = ch * depth + first
                before = buffer[t, pl.ds(at - 1, own), :]
                center = buffer[t, pl.ds(at, own), :]
                after = buffer[t, pl.ds(at + 1, own), :]
                even = fine[ch, t, pl.ds(fine_first, own, stride=2), :] - (before + 6.0 * center + after) * 0.125
                odd = fine[ch, t, pl.ds(fine_first + 1, own, stride=2), :] - (center + after) * 0.5
                out[ch, t, pl.ds(0, own, stride=2), :] = even
                out[ch, t, pl.ds(1, own, stride=2), :] = odd

    first1 = (EDGE - 2) // 2
    count1 = (x.shape[2] - 3 - EDGE) // 2 + first1 + 1
    start1 = EDGE - 2 - 2 * first1
    inner, inner_end, depth1 = 8, rows // 2, v1.shape[1]
    height = inner_end - inner
    reduce_rows(x, v1, start1, height, inner, range(tiles))
    main = product(
        v1[:, pl.ds(inner, height), pl.ds(0, width)].reshape(channels * height, width), w1[pl.ds(0, width), :]
    )
    for ch in range(channels):
        for t in range(l1.shape[1]):
            l1[ch, t, pl.ds(inner, height), :] = main[ch * height:(ch + 1) * height, t * LANES:(t + 1) * LANES]
    each(copy_a, True, lambda c: c.wait_recv())

    lane = lax.broadcasted_iota(jnp.int32, (EDGE, LANES), 1)
    on_right = lane < LANES // 2
    for ch in range(channels):
        gap = jnp.zeros((LANES - 2 * EDGE, rows), F32)
        from_right = jnp.where(right, 0.0, got_r[ch])
        from_left = jnp.where(left, 0.0, got_l[ch])
        x[ch, tiles, pl.ds(EDGE, rows), :] = jnp.concatenate([from_right, gap, from_left], axis=0).T
        for above in (True, False):
            low = corner[3 if above else 1, ch]
            high = corner[2 if above else 0, ch]
            mixed = jnp.where(on_right, jnp.where(right, 0.0, high), jnp.where(left, 0.0, low))
            x[ch, tiles, pl.ds(0 if above else rows + EDGE, EDGE), :] = mixed

    at_ends(x, EDGE, rows, True)
    reduce_rows(x, v1, start1, inner, 0, range(tiles))
    reduce_rows(x, v1, start1, count1 - inner_end, inner_end, range(tiles))
    reduce_rows(x, v1, start1, count1, 0, (tiles,))
    rim = depth1 - height
    outer = jnp.concatenate([v1[:, pl.ds(0, inner), :], v1[:, pl.ds(inner_end, depth1 - inner_end), :]], axis=1)
    outer = product(outer.reshape(channels * rim, v1.shape[2]), w1[...])
    share = product(
        v1[:, pl.ds(inner, height), pl.ds(width, LANES)].reshape(channels * height, LANES), w1[pl.ds(width, LANES), :]
    )
    for ch in range(channels):
        for t in range(l1.shape[1]):
            lanes = slice(t * LANES, (t + 1) * LANES)
            l1[ch, t, pl.ds(0, inner), :] = outer[ch * rim:ch * rim + inner, lanes]
            l1[ch, t, pl.ds(inner_end, depth1 - inner_end), :] = outer[ch * rim + inner:(ch + 1) * rim, lanes]
            l1[ch, t, pl.ds(inner, height), :] += share[ch * height:(ch + 1) * height, lanes]
    at_ends(l1, first1, rows // 2, True)
    reduce_rows(l1, v2, first1 - 2, rows2)
    own = product(
        v2[...].reshape(channels * rows2, v2.shape[2]), w2[...]
    )
    for ch in range(channels):
        l2own[ch] = own[ch * rows2:(ch + 1) * rows2]
        l2[ch, 0, pl.ds(ABOVE, rows2), :] = own[ch * rows2:(ch + 1) * rows2]
    packed = side_l.shape[1]
    filler = jnp.zeros((packed - channels * rows2, LANES), F32)
    flipped = jnp.concatenate([own, filler], axis=0).T
    side_l[...] = flipped[:BELOW]
    side_r[...] = flipped[LANES - ABOVE:]
    each(copy_b, False, lambda c: c.start())

    residual(x, EDGE, l1, first1, rows // 2, e1, exp0, d0)
    fill_weights(w3, col, widths[2], cols[2], widths[3], True, False)
    fill_weights(e2, col, widths[2], cols[2], widths[1], False, True)
    fill_weights(w4, col, widths[3], cols[3], widths[4], True, False)
    fill_weights(w5, col, widths[4], cols[4], widths[5], True, False)
    fill_weights(e3, col, widths[3], cols[3], widths[2], False, True)
    fill_weights(e4, col, widths[4], cols[4], widths[3], False, True)
    fill_weights(e5, col, widths[5], cols[5], widths[4], False, True)
    each(copy_b, True, lambda c: c.wait_recv())

    gap = jnp.zeros((LANES - ABOVE - BELOW, packed), F32)
    parts = ((rows2 - ABOVE, ABOVE, 0), (0, rows2, ABOVE), (0, BELOW, ABOVE + rows2))
    for slot, (take_from, take_count, put_at) in enumerate(parts):
        from_right = jnp.where(right, 0.0, side_got_r[slot])
        from_left = jnp.where(left, 0.0, side_got_l[slot])
        block = jnp.concatenate([from_right, gap, from_left], axis=0).T
        for ch in range(channels):
            at = ch * rows2 + take_from
            l2[ch, 1, pl.ds(put_at, take_count), :] = block[at:at + take_count]

    firsts = [EDGE, first1, ABOVE]
    counts = [None, None, l2.shape[2]]
    residual(l1, first1, l2, ABOVE, rows2, e2, exp1, d1)
    level = l2
    owns = [rows >> k for k in range(LEVELS + 1)]
    stages = ((v3, w3, l3, e3, exp2, d2), (v4, w4, l4, e4, exp3, d3), (v5, w5, l5, e5, exp4, d4))
    for k, (v, w, coarse, e, buffer, out) in enumerate(stages, start=2):
        at_ends(level, firsts[k], owns[k], True)
        first = (firsts[k] - 2) // 2
        count = (counts[k] - 3 - firsts[k]) // 2 + first + 1
        depth = -(-count // 8) * 8
        firsts.append(first)
        counts.append(count)
        for ch in range(channels):
            for t in range(level.shape[1]):
                part = [level[ch, t, pl.ds(firsts[k] - 2 - 2 * first + i, count, stride=2), :] for i in range(5)]
                total = (part[0] + part[4]) * 0.0625 + (part[1] + part[3]) * 0.25 + part[2] * 0.375
                v[ch, pl.ds(0, count), pl.ds(t * LANES, LANES)] = total
        made = product(v[:, pl.ds(0, depth), :].reshape(channels * depth, v.shape[2]), w[...])
        for ch in range(channels):
            coarse[ch, 0] = made[ch * depth:(ch + 1) * depth]
        residual(level, firsts[k], coarse, first, owns[k + 1], e, buffer, out)
        level = coarse
    each(copy_a, False, lambda c: c.wait_send())
    each(copy_b, False, lambda c: c.wait_send())


def solution(mesh):
    def body(x):
        channels, rows, width = x.shape
        image_cols = width * mesh.shape["cols"]
        widths = [width >> k for k in range(LEVELS + 1)]
        p = [pitch(w) for w in widths]
        vm = lambda *shape: pltpu.VMEM(shape, F32)
        wt = lambda *shape: pltpu.VMEM(shape, BF16)
        rows2 = rows // 4
        ext = ABOVE + rows2 + BELOW
        packed = -(-channels * rows2 // LANES) * LANES
        up8 = lambda n: -(-n // 8) * 8
        n1 = up8(rows // 2 + EDGE - 2)
        f3, n3 = (ABOVE - 2) // 2, (ext - 3 - ABOVE) // 2 + (ABOVE - 2) // 2 + 1
        f4, n4 = (f3 - 2) // 2, (n3 - 3 - f3) // 2 + (f3 - 2) // 2 + 1
        n5 = (n4 - 3 - f4) // 2 + (f4 - 2) // 2 + 1
        f5 = (f4 - 2) // 2
        shape = lambda k: jax.ShapeDtypeStruct((channels, rows >> k, width >> k), F32)
        tiled = [(channels, max(widths[k] // LANES, 1), rows >> k, LANES) for k in range(LEVELS)]
        tiled.append((channels, 1, up8(n5), LANES))
        depths = [n1, ext, up8(n3), up8(n4), up8(n5)]
        vmem = pl.BlockSpec(memory_space=pltpu.VMEM)
        anywhere = pl.BlockSpec(memory_space=pl.ANY)
        held = pl.pallas_call(
            functools.partial(kernel, image_cols),
            out_shape=tuple(vm(*dims) for dims in tiled),
            in_specs=[pl.BlockSpec(memory_space=pltpu.HBM)],
            out_specs=(vmem,) * (LEVELS + 1),
            scratch_shapes=[
                vm(channels, p[0] // LANES, rows + 2 * EDGE, LANES),
                vm(channels, EDGE, rows), vm(channels, EDGE, rows),
                vm(channels, EDGE, rows), vm(channels, EDGE, rows),
                vm(4, channels, EDGE, LANES),
                vm(channels, n1, p[0]),
                vm(channels, p[1] // LANES, n1, LANES),
                vm(channels, rows2, LANES),
                vm(channels, p[2] // LANES, ext, LANES),
                vm(BELOW, packed), vm(ABOVE, packed), vm(3, ABOVE, packed), vm(3, BELOW, packed),
                vm(channels, up8(n3), p[2]),
                vm(channels, 1, up8(n3), LANES),
                vm(channels, up8(n4), p[3]),
                vm(channels, 1, up8(n4), LANES),
                vm(channels, up8(n5), p[4]),
                vm(channels, rows2, p[1]),
                *(vm(tiled[k][1], channels * depths[k], LANES) for k in range(LEVELS)),
                wt(p[0], p[1]), wt(p[1], widths[2]), wt(p[2], p[3]), wt(p[3], p[4]), wt(p[4], p[5]),
                wt(p[1], widths[0]), wt(p[2], widths[1]), wt(p[3], LANES), wt(p[4], LANES), wt(p[5], LANES),
                pltpu.SemaphoreType.DMA((width // LANES,)),
                pltpu.SemaphoreType.DMA((8,)), pltpu.SemaphoreType.DMA((8,)),
                pltpu.SemaphoreType.DMA((8,)), pltpu.SemaphoreType.DMA((8,)),
            ],
            compiler_params=pltpu.CompilerParams(collective_id=0, has_side_effects=True),
            name="pyramid",
        )(x)
        copies = sum(dims[1] for dims in tiled[:3])
        return pl.pallas_call(
            functools.partial(hand_out, f5),
            out_shape=tuple(shape(k) for k in range(LEVELS + 1)),
            in_specs=[anywhere] * 3 + [vmem] * 3,
            out_specs=(anywhere,) * 3 + (vmem,) * 3,
            scratch_shapes=[pltpu.SemaphoreType.DMA((copies,))],
            compiler_params=pltpu.CompilerParams(vmem_limit_bytes=VMEM_GRANT),
            name="hand_out",
        )(*(pltpu.with_memory_space_constraint(part, pltpu.VMEM) for part in held))

    placed = P(None, "rows", "cols")
    return jax.shard_map(
        body, mesh=mesh, in_specs=(placed,), out_specs=(placed,) * (LEVELS + 1), check_vma=False
    )
```
